32 devices in a mesh: dp: 4 (over x, y), tp: 8 (over z, core).
Axes of the slice: x: 2, y: 2, z: 4, core: 2. Of those that a mesh axis runs over, the one named last changes fastest.
Arguments:
- x: bfloat16 [16384, 2048], P(('dp', 'tp')), parts along dimension 0
- dy: bfloat16 [16384, 2048], P(('dp', 'tp')), parts along dimension 0
- gate: bfloat16 [16384, 8192], P('dp', 'tp'), parts along dimension 0
- up: bfloat16 [16384, 8192], P('dp', 'tp'), parts along dimension 0
- w_gate: bfloat16 [2048, 8192], P(None, 'tp')
- w_up: bfloat16 [2048, 8192], P(None, 'tp')
- w_down: bfloat16 [8192, 2048], P('tp')
Outputs:
- output 1: bfloat16 [16384, 2048], P(('dp', 'tp')), parts along dimension 0
- output 2: bfloat16 [8192, 8192], P('dp', 'tp'), parts along dimension 0
- output 3: bfloat16 [8192, 8192], P('dp', 'tp'), parts along dimension 0
- output 4: bfloat16 [32768, 2048], P(('dp', 'tp')), parts along dimension 0
There are 4 independent parts. The reference program is written for one: setup_inputs(seed, part) draws one part's arguments, and reference() takes and returns one part's arrays. A program takes and returns all parts, laid end to end along the dimension named above; an argument that names none is the same for every part.
All inputs are finite; a program needn't handle non-finite values.
Results may differ from the reference program's by a relative error of at most 0.012.
Values are sent between devices in bfloat16 or wider.
A program may use at most 2 GiB of HBM per device.

```python
import jax
import jax.numpy as jnp

ROWS = 4096
D = 2048
FF = 8192


def act(gate, up):
    return jax.nn.silu(gate) * up


def setup_inputs(seed: int = 0, part: int = 0) -> dict:
    kx, ky, ka, kb, kg, ku, kd = jax.random.split(jax.random.key(seed), 7)
    kx, ky, ka, kb = (jax.random.fold_in(k, part) for k in (kx, ky, ka, kb))
    drawn = {
        "x": jax.random.normal(kx, (ROWS, D), jnp.float32),
        "dy": jax.random.normal(ky, (ROWS, D), jnp.float32),
        "gate": jax.random.normal(ka, (ROWS, FF), jnp.float32),
        "up": jax.random.normal(kb, (ROWS, FF), jnp.float32),
        "w_gate": jax.random.normal(kg, (D, FF), jnp.float32) * D**-0.5,
        "w_up": jax.random.normal(ku, (D, FF), jnp.float32) * D**-0.5,
        "w_down": jax.random.normal(kd, (FF, D), jnp.float32) * FF**-0.5,
    }
    return {k: v.astype(jnp.bfloat16) for k, v in drawn.items()}


def reference(x, dy, gate, up, w_gate, w_up, w_down):
    hidden, back = jax.vjp(act, gate.astype(jnp.float32), up.astype(jnp.float32))
    d_hidden = jnp.dot(dy, w_down.T, preferred_element_type=jnp.float32)
    d_gate, d_up = (g.astype(jnp.bfloat16) for g in back(d_hidden))
    dx = jnp.dot(d_gate, w_gate.T, preferred_element_type=jnp.float32) + jnp.dot(d_up, w_up.T, preferred_element_type=jnp.float32)
    dw_gate = jnp.dot(x.T, d_gate, preferred_element_type=jnp.float32)
    dw_up = jnp.dot(x.T, d_up, preferred_element_type=jnp.float32)
    dw_down = jnp.dot(hidden.astype(jnp.bfloat16).T, dy, preferred_element_type=jnp.float32)
    return tuple(g.astype(jnp.bfloat16) for g in (dx, dw_gate, dw_up, dw_down))
```

```python
import functools

import jax
import jax.numpy as jnp
from jax import lax
from jax.experimental import pallas as pl
from jax.experimental.pallas import tpu as pltpu
from jax.sharding import PartitionSpec as P

MESH = pl.DeviceIdType.MESH
CHUNKS = 2
TILE = 256
CHIPS = 4
NT = (((1,), (1,)), ((), ()))
TN = (((0,), (0,)), ((), ()))
X, FORWARD, REDUCE, WRITE_GU, WRITE_DOWN = range(5)
END_STEPS = (
    (REDUCE, 0), (REDUCE, 1), (WRITE_DOWN, 0), (X, 0), (X, 1), (FORWARD, 1), (X, 2), (X, 3), (REDUCE, 2),
    (FORWARD, 2), (X, 4), (X, 5), (FORWARD, 3), (X, 6), (X, 7), (WRITE_GU, 0), (REDUCE, 3),
)
MIDDLE_STEPS = (
    (WRITE_DOWN, 0), (X, 0), (X, 1), (FORWARD, 1), (X, 2), (X, 3), (X, 4), (X, 5), (FORWARD, 2),
    (X, 6), (X, 7), (FORWARD, 3), (REDUCE, 0), (REDUCE, 1), (REDUCE, 2), (WRITE_GU, 0), (REDUCE, 3),
)


def pick(table, i):
    value = jnp.int32(table[0])
    for j in range(1, len(table)):
        value = jnp.where(i == j, jnp.int32(table[j]), value)
    return value


def dot(a, b, dims):
    return lax.dot_general(a, b, dims, preferred_element_type=jnp.float32)


def kernel(
    x, dy, gate, up, w_gate, w_up, w_down,
    dx, dw_gate, dw_up, dw_down, dy_all, x_all, from_partner, from_below, from_above,
    wg, wu, wd, dg, du, acc1, acc2, tok, gv, uv, hid, st,
    w_sem, tok_sem, gate_sem, out_sem, recv_sem, send_sem, partner_sem, below_sem, above_sem, st_sem,
):
    rows, depth = x.shape
    width = gate.shape[1]
    part = rows // CHUNKS
    me = lax.axis_index("tp")
    z, c = me // 2, lax.rem(me, 2)
    other = 1 - c
    last = CHIPS - 1
    is_end = (z == 0) | (z == last)
    low = z < CHIPS // 2
    has_below, has_above = z > 0, z < last
    partner, below, above = {"tp": 2 * z + other}, {"tp": 2 * (z - 1) + c}, {"tp": 2 * (z + 1) + c}

    def mirrored(v):
        return jnp.where(low, v, last - v)

    def arrival(k):
        return mirrored(jnp.where(is_end, k, pick((1, 2, 0, 3), k)))

    def target(r):
        return mirrored(jnp.where(is_end, last - r, pick((3, 0, 2, 1), r)))

    def block_rows(b):
        return pl.ds(pl.multiple_of(b * rows, rows), rows)

    def chunk_rows(b, h):
        return pl.ds(pl.multiple_of(b * rows + h * part, part), part)

    def tile(i, size=TILE):
        return pl.ds(pl.multiple_of(i * size, size), size)

    own = (dy, x)
    whole = (dy_all, x_all)

    def send(t, way, chip, h, device, mine):
        b = 2 * chip + c
        src = own[t].at[pl.ds(h * part, part)] if mine else whole[t].at[chunk_rows(b, h)]
        return pltpu.make_async_remote_copy(
            src_ref=src,
            dst_ref=whole[t].at[chunk_rows(b, h)],
            send_sem=send_sem.at[t, way, chip, h],
            recv_sem=recv_sem.at[t, b, h],
            device_id=device,
            device_id_type=MESH,
        )

    def await_chunk(t, b, h):
        pltpu.make_async_remote_copy(
            src_ref=whole[t].at[chunk_rows(b, h)],
            dst_ref=whole[t].at[chunk_rows(b, h)],
            send_sem=send_sem.at[t, 0, 0, h],
            recv_sem=recv_sem.at[t, b, h],
            device_id=partner,
            device_id_type=MESH,
        ).wait_recv()

    def send_own(t, ways):
        for h in range(CHUNKS):
            for way, device in enumerate((above, below, partner)):
                if ways[way] is True:
                    send(t, way, z, h, device, True).start()
                elif ways[way] is not False:
                    pl.when(ways[way])(lambda t=t, way=way, h=h, device=device: send(t, way, z, h, device, True).start())

    def forward(t, k):
        for h in range(CHUNKS):
            @pl.when(z - k >= 0)
            def _():
                chip = z - k
                await_chunk(t, 2 * chip + c, h)
                pl.when(has_above)(lambda: send(t, 0, chip, h, above, False).start())
                send(t, 2, chip, h, partner, False).start()

            @pl.when(z + k <= last)
            def _():
                chip = z + k
                await_chunk(t, 2 * chip + c, h)
                pl.when(has_below)(lambda: send(t, 1, chip, h, below, False).start())
                send(t, 2, chip, h, partner, False).start()

    def send_x_after(k):
        send_own(1, (has_above & (z == k), has_below & (last - z == k), False))

    barrier = pltpu.get_barrier_semaphore()
    pl.semaphore_signal(barrier, inc=1, device_id=partner, device_id_type=MESH)
    pl.when(has_below)(lambda: pl.semaphore_signal(barrier, inc=1, device_id=below, device_id_type=MESH))
    pl.when(has_above)(lambda: pl.semaphore_signal(barrier, inc=1, device_id=above, device_id_type=MESH))
    pl.semaphore_wait(barrier, jnp.where(is_end, 2, 3))
    send_own(0, (has_above, has_below, True))
    send_x_after(0)
    send_own(1, (False, False, True))

    weights = [pltpu.make_async_copy(a, b, w_sem.at[i]) for i, (a, b) in enumerate(((w_down, wd), (w_gate, wg), (w_up, wu)))]
    for copy in weights:
        copy.start()

    def gate_up(s):
        b = 2 * arrival(s // 2) + jnp.where(lax.rem(s, 2) == 0, c, other)
        slot = lax.rem(s, 2)
        return (
            pltpu.make_async_copy(gate.at[block_rows(b)], gv.at[slot], gate_sem.at[0, slot]),
            pltpu.make_async_copy(up.at[block_rows(b)], uv.at[slot], gate_sem.at[1, slot]),
        )

    for copy in gate_up(jnp.int32(0)):
        copy.start()

    @pl.loop(0, acc1.shape[0] // TILE)
    def _(i):
        acc1[tile(i), :] = jnp.zeros((TILE, width), jnp.float32)

    for copy in weights:
        copy.wait()

    def take_tokens(t, s, b, slot):
        @pl.when(lax.rem(s, 2) == 1)
        def _():
            for h in range(CHUNKS):
                await_chunk(t, b, h)

        @pl.when(s == 0)
        def _():
            pltpu.make_async_copy(own[t], tok.at[slot], tok_sem).start()

        @pl.when(s > 0)
        def _():
            pltpu.make_async_copy(whole[t].at[block_rows(b)], tok.at[slot], tok_sem).start()

        pltpu.make_async_copy(own[t], tok.at[slot], tok_sem).wait()

    def partner_send(chip, h, slot):
        return pltpu.make_async_remote_copy(
            src_ref=st.at[slot],
            dst_ref=from_partner.at[chip, pl.ds(h * part, part)],
            send_sem=st_sem.at[slot],
            recv_sem=partner_sem.at[chip, h],
            device_id=partner,
            device_id_type=MESH,
        )

    @pl.loop(0, 2 * CHIPS)
    def _(s):
        k, odd = s // 2, lax.rem(s, 2)
        chip = arrival(k)
        b = 2 * chip + jnp.where(odd == 0, c, other)
        slot = odd

        for j in range(1, CHIPS):
            @pl.when(s == 2 * j)
            def _(j=j):
                forward(0, j)
                send_x_after(j)

        take_tokens(0, s, b, slot)

        @pl.when(s + 1 < 2 * CHIPS)
        def _():
            for copy in gate_up(s + 1):
                copy.start()

        for copy in gate_up(s):
            copy.wait()

        @pl.loop(0, width // TILE)
        def _(i):
            cols = tile(i)
            d_hidden = dot(tok[slot], wd[cols, :], NT)
            g = gv[slot, :, cols].astype(jnp.float32)
            u = uv[slot, :, cols].astype(jnp.float32)
            s_ = jax.nn.sigmoid(g)
            silu = g * s_
            hid[:, cols] = (silu * u).astype(jnp.bfloat16)
            du[block_rows(b), cols] = (d_hidden * silu).astype(jnp.bfloat16)
            dg[block_rows(b), cols] = (d_hidden * u * (s_ * (1.0 + g * (1.0 - s_)))).astype(jnp.bfloat16)

        @pl.loop(0, width // TILE)
        def _(i):
            left = hid[:, tile(i)]
            acc1[tile(i), :] += dot(left, tok[slot, :, :width], TN)
            acc1[pl.ds(pl.multiple_of(width + i * TILE, TILE), TILE), :] += dot(left, tok[slot, :, width:], TN)

        @pl.when(odd == 1)
        def _():
            base = 2 * lax.rem(k, 2)

            @pl.when(k >= 2)
            def _():
                for h in range(CHUNKS):
                    partner_send(chip, h, base + h).wait_send()

            @pl.loop(0, depth // TILE)
            def _(i):
                term = dot(dg[block_rows(b), :], wg[tile(i), :], NT) + dot(du[block_rows(b), :], wu[tile(i), :], NT)
                for h in range(CHUNKS):
                    st[base + h, :, tile(i)] = term[h * part:(h + 1) * part].astype(jnp.bfloat16)

            for h in range(CHUNKS):
                partner_send(chip, h, base + h).start()

    def x_step(s):
        chip = arrival(s // 2)
        b = 2 * chip + jnp.where(lax.rem(s, 2) == 0, c, other)
        slot = lax.rem(s, 2)
        take_tokens(1, s, b, slot)

        @pl.loop(0, depth // TILE)
        def _(i):
            left = tok[slot, :, tile(i)]
            acc1[tile(i), :] += dot(left, dg[block_rows(b), :], TN)
            acc2[tile(i), :] += dot(left, du[block_rows(b), :], TN)

    def incoming(buffer, sem, chip, h, j):
        piece = buffer.at[chip, tile(h, part)]
        pltpu.make_async_remote_copy(
            src_ref=piece, dst_ref=piece, send_sem=st_sem.at[0], recv_sem=sem.at[chip, h], device_id=partner, device_id_type=MESH
        ).wait_recv()
        copy = pltpu.make_async_copy(piece, wd.at[pl.ds(j * part, part)], tok_sem)
        copy.start()
        copy.wait()

    def reduce_step(r):
        chip = target(r)
        b = 2 * chip + c

        @pl.loop(0, CHUNKS)
        def _(h):
            slot = 2 * lax.rem(r, 2) + h
            partner_send(chip, 0, slot).wait_send()
            incoming(from_partner, partner_sem, chip, h, 0)
            use_below, use_above = (chip >= z) & has_below, (chip <= z) & has_above
            for j, (use, buffer, sem) in enumerate(((use_below, from_below, below_sem), (use_above, from_above, above_sem)), 1):
                pl.when(use)(lambda j=j, buffer=buffer, sem=sem: incoming(buffer, sem, chip, h, j))

                @pl.when(jnp.logical_not(use))
                def _(j=j):
                    wd[j * part:(j + 1) * part, :] = jnp.zeros((part, depth), jnp.bfloat16)

            @pl.loop(0, depth // TILE)
            def _(i):
                here = chunk_rows(b, h)
                total = dot(dg[here, :], wg[tile(i), :], NT) + dot(du[here, :], wu[tile(i), :], NT)
                for j in range(3):
                    total += wd[j * part:(j + 1) * part, tile(i)].astype(jnp.float32)
                st[slot, :, tile(i)] = total.astype(jnp.bfloat16)

            def pass_on(buffer, sem, device):
                pltpu.make_async_remote_copy(
                    src_ref=st.at[slot],
                    dst_ref=buffer.at[chip, tile(h, part)],
                    send_sem=st_sem.at[slot],
                    recv_sem=sem.at[chip, h],
                    device_id=device,
                    device_id_type=MESH,
                ).start()

            pl.when(chip > z)(lambda: pass_on(from_below, below_sem, above))
            pl.when(chip < z)(lambda: pass_on(from_above, above_sem, below))
            pl.when(chip == z)(lambda: pltpu.make_async_copy(st.at[slot], dx.at[tile(h, part)], st_sem.at[slot]).start())

    half = depth // 2
    stage = [gv.at[0], gv.at[1], uv.at[0], uv.at[1]]

    def down_copy(q):
        span = width // 2
        return pltpu.make_async_copy(
            stage[q], dw_down.at[pl.ds((q % 2) * span, span), pl.ds((q // 2) * width, width)], out_sem.at[2 + q]
        )

    def write_down():
        for q in range(4):
            span = width // 2
            stage[q][...] = acc1[q * span:(q + 1) * span, :].astype(jnp.bfloat16)
            down_copy(q).start()

        @pl.loop(0, depth // TILE)
        def _(i):
            acc1[tile(i), :] = jnp.zeros((TILE, width), jnp.float32)
            acc2[tile(i), :] = jnp.zeros((TILE, width), jnp.float32)

    free = jnp.where(low, depth, 0)

    def gu_copies():
        span = pl.ds(pl.multiple_of(free, depth), depth)
        return (
            pltpu.make_async_copy(dg.at[span], dw_gate, out_sem.at[0]),
            pltpu.make_async_copy(du.at[span], dw_up, out_sem.at[1]),
        )

    def write_gu():
        @pl.loop(0, depth // TILE)
        def _(i):
            there = pl.ds(pl.multiple_of(free + i * TILE, TILE), TILE)
            dg[there, :] = acc1[tile(i), :].astype(jnp.bfloat16)
            du[there, :] = acc2[tile(i), :].astype(jnp.bfloat16)

        for copy in gu_copies():
            copy.start()

    @pl.loop(0, len(END_STEPS))
    def _(t):
        kind = jnp.where(is_end, pick([s[0] for s in END_STEPS], t), pick([s[0] for s in MIDDLE_STEPS], t))
        arg = jnp.where(is_end, pick([s[1] for s in END_STEPS], t), pick([s[1] for s in MIDDLE_STEPS], t))
        pl.when(kind == X)(lambda: x_step(arg))
        for k in range(1, CHIPS):
            pl.when((kind == FORWARD) & (arg == k))(lambda k=k: forward(1, k))
        pl.when(kind == REDUCE)(lambda: reduce_step(arg))
        pl.when(kind == WRITE_GU)(write_gu)
        pl.when(kind == WRITE_DOWN)(write_down)

    for q in range(4):
        down_copy(q).wait()
    for copy in gu_copies():
        copy.wait()
    for slot in range(2 * CHUNKS):
        partner_send(0, 0, slot).wait_send()
    for t in range(2):
        @pl.loop(0, CHIPS)
        def _(chip, t=t):
            for h in range(CHUNKS):
                pl.when(has_above & (chip <= z))(lambda h=h: send(t, 0, chip, h, partner, False).wait_send())
                pl.when(has_below & (chip >= z))(lambda h=h: send(t, 1, chip, h, partner, False).wait_send())
                send(t, 2, chip, h, partner, False).wait_send()


def solution(mesh):
    def step(x, dy, gate, up, w_gate, w_up, w_down):
        rows, depth = x.shape
        tokens, width = gate.shape
        bf16 = jnp.bfloat16
        part = rows // CHUNKS
        hbm = pl.BlockSpec(memory_space=pl.ANY)
        shapes = [
            (rows, depth), (depth, width), (depth, width), (width, depth),
            (tokens, depth), (tokens, depth), (CHIPS, rows, depth), (CHIPS, rows, depth), (CHIPS, rows, depth),
        ]
        dma = pltpu.SemaphoreType.DMA
        out = pl.pallas_call(
            kernel,
            out_shape=[jax.ShapeDtypeStruct(s, bf16) for s in shapes],
            in_specs=[hbm] * 7,
            out_specs=[hbm] * len(shapes),
            scratch_shapes=[
                pltpu.VMEM((depth, width), bf16), pltpu.VMEM((depth, width), bf16), pltpu.VMEM((width, depth), bf16),
                pltpu.VMEM((tokens, width), bf16), pltpu.VMEM((tokens, width), bf16),
                pltpu.VMEM((depth, width), jnp.float32), pltpu.VMEM((depth, width), jnp.float32),
                pltpu.VMEM((2, rows, depth), bf16),
                pltpu.VMEM((2, rows, width), bf16), pltpu.VMEM((2, rows, width), bf16), pltpu.VMEM((rows, width), bf16),
                pltpu.VMEM((2 * CHUNKS, part, depth), bf16),
                dma((3,)), dma, dma((2, 2)), dma((6,)),
                dma((2, 2 * CHIPS, CHUNKS)), dma((2, 3, CHIPS, CHUNKS)),
                dma((CHIPS, CHUNKS)), dma((CHIPS, CHUNKS)), dma((CHIPS, CHUNKS)), dma((2 * CHUNKS,)),
            ],
            compiler_params=pltpu.CompilerParams(collective_id=0, has_side_effects=True, vmem_limit_bytes=67043328),
            cost_estimate=pl.CostEstimate(flops=12 * tokens * depth * width, bytes_accessed=150 * 2**20, transcendentals=0),
        )(x, dy, gate, up, w_gate, w_up, w_down)
        return tuple(out[:4])

    whole, rows, cols = P(("dp", "tp"), None), P("tp", None), P(None, "tp")
    return jax.shard_map(
        step,
        mesh=mesh,
        in_specs=(whole, whole, P("dp", "tp"), P("dp", "tp"), cols, cols, rows),
        out_specs=(whole, P("dp", "tp"), P("dp", "tp"), whole),
        check_vma=False,
    )
```

```python
import functools

import jax
import jax.numpy as jnp
from jax import lax
from jax.experimental import pallas as pl
from jax.experimental.pallas import tpu as pltpu
from jax.sharding import PartitionSpec as P

MESH = pl.DeviceIdType.MESH
CHUNKS = 2
PIECES = 2
TILE = 256
CHIPS = 4
NT = (((1,), (1,)), ((), ()))
TN = (((0,), (0,)), ((), ()))
X, FORWARD, REDUCE, WRITE_GU, WRITE_DOWN, OWN, FINISH = range(7)
END_STEPS = (
    (REDUCE, 0), (REDUCE, 1), (WRITE_DOWN, 0), (X, 0), (X, 1), (FORWARD, 1), (X, 2), (X, 3), (REDUCE, 2),
    (FORWARD, 2), (X, 4), (X, 5), (FORWARD, 3), (X, 6), (X, 7), (WRITE_GU, 0), (OWN, 0), (FINISH, 0),
)
MIDDLE_STEPS = (
    (WRITE_DOWN, 0), (X, 0), (X, 1), (FORWARD, 1), (X, 2), (X, 3), (X, 4), (X, 5), (FORWARD, 2),
    (X, 6), (X, 7), (FORWARD, 3), (REDUCE, 0), (REDUCE, 1), (REDUCE, 2), (WRITE_GU, 0), (OWN, 0), (FINISH, 0),
)


def pick(table, i):
    value = jnp.int32(table[0])
    for j in range(1, len(table)):
        value = jnp.where(i == j, jnp.int32(table[j]), value)
    return value


def dot(a, b, dims):
    return lax.dot_general(a, b, dims, preferred_element_type=jnp.float32)


def free_rows(depth):
    z = lax.axis_index("tp") // 2
    return pl.multiple_of(jnp.where(z < CHIPS // 2, depth, 0), depth)


def kernel(
    x, dy, gate, up, w_gate, w_up, w_down,
    dx, dg, du, wd, dy_all, x_all, from_partner, from_below, from_above,
    wg, wu, acc1, acc2, tok, gv, uv, hid, st, terms,
    w_sem, tok_sem, gate_sem, recv_sem, send_sem, partner_sem, below_sem, above_sem, st_sem,
):
    rows, depth = x.shape
    width = gate.shape[1]
    part = rows // CHUNKS
    me = lax.axis_index("tp")
    z, c = me // 2, lax.rem(me, 2)
    other = 1 - c
    last = CHIPS - 1
    is_end = (z == 0) | (z == last)
    low = z < CHIPS // 2
    has_below, has_above = z > 0, z < last
    partner, below, above = {"tp": 2 * z + other}, {"tp": 2 * (z - 1) + c}, {"tp": 2 * (z + 1) + c}

    def mirrored(v):
        return jnp.where(low, v, last - v)

    def arrival(k):
        return mirrored(jnp.where(is_end, k, pick((1, 2, 0, 3), k)))

    def target(r):
        return mirrored(jnp.where(is_end, last - r, pick((3, 0, 2, 1), r)))

    def block_rows(b):
        return pl.ds(pl.multiple_of(b * rows, rows), rows)

    def chunk_rows(b, h):
        return pl.ds(pl.multiple_of(b * rows + h * part, part), part)

    def tile(i, size=TILE):
        return pl.ds(pl.multiple_of(i * size, size), size)

    own = (dy, x)
    whole = (dy_all, x_all)

    def send(t, way, chip, h, device, mine):
        b = 2 * chip + c
        src = own[t].at[pl.ds(h * part, part)] if mine else whole[t].at[chunk_rows(b, h)]
        return pltpu.make_async_remote_copy(
            src_ref=src,
            dst_ref=whole[t].at[chunk_rows(b, h)],
            send_sem=send_sem.at[t, way, chip, h],
            recv_sem=recv_sem.at[t, b, h],
            device_id=device,
            device_id_type=MESH,
        )

    def await_chunk(t, b, h):
        pltpu.make_async_remote_copy(
            src_ref=whole[t].at[chunk_rows(b, h)],
            dst_ref=whole[t].at[chunk_rows(b, h)],
            send_sem=send_sem.at[t, 0, 0, h],
            recv_sem=recv_sem.at[t, b, h],
            device_id=partner,
            device_id_type=MESH,
        ).wait_recv()

    def send_own(t, ways):
        for h in range(CHUNKS):
            for way, device in enumerate((above, below, partner)):
                if ways[way] is True:
                    send(t, way, z, h, device, True).start()
                elif ways[way] is not False:
                    pl.when(ways[way])(lambda t=t, way=way, h=h, device=device: send(t, way, z, h, device, True).start())

    def forward(t, k):
        for h in range(CHUNKS):
            @pl.when(z - k >= 0)
            def _():
                chip = z - k
                await_chunk(t, 2 * chip + c, h)
                pl.when(has_above)(lambda: send(t, 0, chip, h, above, False).start())
                send(t, 2, chip, h, partner, False).start()

            @pl.when(z + k <= last)
            def _():
                chip = z + k
                await_chunk(t, 2 * chip + c, h)
                pl.when(has_below)(lambda: send(t, 1, chip, h, below, False).start())
                send(t, 2, chip, h, partner, False).start()

    def send_x_after(k):
        send_own(1, (has_above & (z == k), has_below & (last - z == k), False))

    barrier = pltpu.get_barrier_semaphore()
    pl.semaphore_signal(barrier, inc=1, device_id=partner, device_id_type=MESH)
    pl.when(has_below)(lambda: pl.semaphore_signal(barrier, inc=1, device_id=below, device_id_type=MESH))
    pl.when(has_above)(lambda: pl.semaphore_signal(barrier, inc=1, device_id=above, device_id_type=MESH))
    pl.semaphore_wait(barrier, jnp.where(is_end, 2, 3))
    send_own(0, (has_above, has_below, True))
    send_x_after(0)
    send_own(1, (False, False, True))

    weights = [pltpu.make_async_copy(a, b, w_sem.at[i]) for i, (a, b) in enumerate(((w_down, wd), (w_gate, wg), (w_up, wu)))]
    for copy in weights:
        copy.start()

    def gate_up(s):
        b = 2 * arrival(s // 2) + jnp.where(lax.rem(s, 2) == 0, c, other)
        slot = lax.rem(s, 2)
        return (
            pltpu.make_async_copy(gate.at[block_rows(b)], gv.at[slot], gate_sem.at[0, slot]),
            pltpu.make_async_copy(up.at[block_rows(b)], uv.at[slot], gate_sem.at[1, slot]),
        )

    for copy in gate_up(jnp.int32(0)):
        copy.start()

    @pl.loop(0, acc1.shape[0] // TILE)
    def _(i):
        acc1[tile(i), :] = jnp.zeros((TILE, width), jnp.float32)

    for copy in weights:
        copy.wait()

    def take_tokens(t, s, b):
        @pl.when(lax.rem(s, 2) == 1)
        def _():
            for h in range(CHUNKS):
                await_chunk(t, b, h)

        @pl.when(s == 0)
        def _():
            pltpu.make_async_copy(own[t], tok, tok_sem).start()

        @pl.when(s > 0)
        def _():
            pltpu.make_async_copy(whole[t].at[block_rows(b)], tok, tok_sem).start()

        pltpu.make_async_copy(own[t], tok, tok_sem).wait()

    def partner_send(chip, h, slot):
        return pltpu.make_async_remote_copy(
            src_ref=st.at[slot],
            dst_ref=from_partner.at[chip, pl.ds(h * part, part)],
            send_sem=st_sem.at[slot],
            recv_sem=partner_sem.at[chip, h],
            device_id=partner,
            device_id_type=MESH,
        )

    @pl.loop(0, 2 * CHIPS)
    def _(s):
        k, odd = s // 2, lax.rem(s, 2)
        chip = arrival(k)
        b = 2 * chip + jnp.where(odd == 0, c, other)
        slot = odd

        for j in range(1, CHIPS):
            @pl.when(s == 2 * j)
            def _(j=j):
                forward(0, j)
                send_x_after(j)

        take_tokens(0, s, b)

        @pl.when(s + 1 < 2 * CHIPS)
        def _():
            for copy in gate_up(s + 1):
                copy.start()

        for copy in gate_up(s):
            copy.wait()

        @pl.loop(0, width // TILE)
        def _(i):
            cols = tile(i)
            d_hidden = dot(tok[...], wd[cols, :], NT)
            g = gv[slot, :, cols].astype(jnp.float32)
            u = uv[slot, :, cols].astype(jnp.float32)
            s_ = jax.nn.sigmoid(g)
            silu = g * s_
            hid[:, cols] = (silu * u).astype(jnp.bfloat16)
            du[block_rows(b), cols] = (d_hidden * silu).astype(jnp.bfloat16)
            dg[block_rows(b), cols] = (d_hidden * u * (s_ * (1.0 + g * (1.0 - s_)))).astype(jnp.bfloat16)

        @pl.loop(0, width // TILE)
        def _(i):
            left = hid[:, tile(i)]
            acc1[tile(i), :] += dot(left, tok[:, :width], TN)
            acc1[pl.ds(pl.multiple_of(width + i * TILE, TILE), TILE), :] += dot(left, tok[:, width:], TN)

        @pl.when(odd == 1)
        def _():
            base = 2 * lax.rem(k, 2)

            @pl.when(k >= 2)
            def _():
                for h in range(CHUNKS):
                    partner_send(chip, h, base + h).wait_send()

            @pl.loop(0, depth // TILE)
            def _(i):
                term = dot(dg[block_rows(b), :], wg[tile(i), :], NT) + dot(du[block_rows(b), :], wu[tile(i), :], NT)
                for h in range(CHUNKS):
                    st[base + h, :, tile(i)] = term[h * part:(h + 1) * part].astype(jnp.bfloat16)

            for h in range(CHUNKS):
                partner_send(chip, h, base + h).start()

    def x_step(s):
        chip = arrival(s // 2)
        b = 2 * chip + jnp.where(lax.rem(s, 2) == 0, c, other)
        take_tokens(1, s, b)

        @pl.loop(0, depth // TILE)
        def _(i):
            left = tok[:, tile(i)]
            acc1[tile(i), :] += dot(left, dg[block_rows(b), :], TN)
            acc2[tile(i), :] += dot(left, du[block_rows(b), :], TN)

    fine = part // PIECES

    def arrived(buffer, sem, chip, at, size):
        piece = buffer.at[chip, pl.ds(pl.multiple_of(at * size, size), size)]
        pltpu.make_async_remote_copy(
            src_ref=piece, dst_ref=piece, send_sem=st_sem.at[0], recv_sem=sem.at[chip, at], device_id=partner, device_id_type=MESH
        ).wait_recv()

    def take_term(buffer, chip, at, size, j):
        copy = pltpu.make_async_copy(
            buffer.at[chip, pl.ds(pl.multiple_of(at * size, size), size)], terms.at[j, pl.ds(0, size)], tok_sem
        )
        copy.start()
        copy.wait()

    def own_term(b, h, i):
        here = chunk_rows(b, h)
        return dot(dg[here, :], wg[tile(i), :], NT) + dot(du[here, :], wu[tile(i), :], NT)

    def reduce_step(r):
        chip = target(r)
        b = 2 * chip + c

        @pl.loop(0, CHUNKS)
        def _(h):
            slot = 2 * lax.rem(r, 2) + h
            partner_send(chip, 0, slot).wait_send()
            arrived(from_partner, partner_sem, chip, h, part)
            take_term(from_partner, chip, h, part, 0)
            going_up = chip > z
            for use, buffer, sem in (
                (going_up & has_below, from_below, below_sem),
                (jnp.logical_not(going_up) & has_above, from_above, above_sem),
            ):
                @pl.when(use)
                def _(buffer=buffer, sem=sem):
                    for q in range(PIECES):
                        arrived(buffer, sem, chip, PIECES * h + q, fine)
                    take_term(buffer, chip, h, part, 1)

            @pl.when(is_end)
            def _():
                terms[1] = jnp.zeros((part, depth), jnp.bfloat16)

            @pl.loop(0, depth // TILE)
            def _(i):
                total = own_term(b, h, i)
                for j in range(2):
                    total += terms[j, :, tile(i)].astype(jnp.float32)
                st[slot, :, tile(i)] = total.astype(jnp.bfloat16)

            def pass_on(buffer, sem, device):
                for q in range(PIECES):
                    at = PIECES * h + q
                    pltpu.make_async_remote_copy(
                        src_ref=st.at[slot, pl.ds(q * fine, fine)],
                        dst_ref=buffer.at[chip, pl.ds(pl.multiple_of(at * fine, fine), fine)],
                        send_sem=st_sem.at[slot],
                        recv_sem=sem.at[chip, at],
                        device_id=device,
                        device_id_type=MESH,
                    ).start()

            pl.when(going_up)(lambda: pass_on(from_below, below_sem, above))
            pl.when(jnp.logical_not(going_up))(lambda: pass_on(from_above, above_sem, below))

    def halves(i):
        return lax.rem(i, width // TILE), (i // (width // TILE)) * rows

    def own_step():
        @pl.loop(0, CHUNKS)
        def _(h):
            arrived(from_partner, partner_sem, z, h, part)
            take_term(from_partner, z, h, part, 0)

            @pl.loop(0, depth // TILE)
            def _(i):
                column, down = halves(i)
                total = own_term(me, h, i) + terms[0, :, tile(i)].astype(jnp.float32)
                acc1[pl.ds(pl.multiple_of(down + h * part, part), part), tile(column)] = total

    def finish():
        for at in range(CHUNKS * PIECES):
            for j, (use, buffer, sem) in enumerate(((has_below, from_below, below_sem), (has_above, from_above, above_sem))):
                @pl.when(use)
                def _(j=j, buffer=buffer, sem=sem):
                    arrived(buffer, sem, z, at, fine)
                    take_term(buffer, z, at, fine, j)
                    for side in range(2):
                        here = pl.ds(side * rows + at * fine, fine)
                        acc1[here, :] += terms[j, :fine, side * width:(side + 1) * width].astype(jnp.float32)
            for side in range(2):
                here = pl.ds(side * rows + at * fine, fine)
                dx[at * fine:(at + 1) * fine, side * width:(side + 1) * width] = acc1[here, :].astype(jnp.bfloat16)

    def write_down():
        for side in range(2):
            wd[:, side * width:(side + 1) * width] = acc1[side * width:(side + 1) * width, :].astype(jnp.bfloat16)

        @pl.loop(0, depth // TILE)
        def _(i):
            acc1[tile(i), :] = jnp.zeros((TILE, width), jnp.float32)
            acc2[tile(i), :] = jnp.zeros((TILE, width), jnp.float32)

    def write_gu():
        free = free_rows(depth)

        @pl.loop(0, depth // TILE)
        def _(i):
            there = pl.ds(pl.multiple_of(free + i * TILE, TILE), TILE)
            dg[there, :] = acc1[tile(i), :].astype(jnp.bfloat16)
            du[there, :] = acc2[tile(i), :].astype(jnp.bfloat16)

    @pl.loop(0, len(END_STEPS))
    def _(t):
        kind = jnp.where(is_end, pick([s[0] for s in END_STEPS], t), pick([s[0] for s in MIDDLE_STEPS], t))
        arg = jnp.where(is_end, pick([s[1] for s in END_STEPS], t), pick([s[1] for s in MIDDLE_STEPS], t))
        pl.when(kind == X)(lambda: x_step(arg))
        for k in range(1, CHIPS):
            pl.when((kind == FORWARD) & (arg == k))(lambda k=k: forward(1, k))
        pl.when(kind == REDUCE)(lambda: reduce_step(arg))
        pl.when(kind == WRITE_GU)(write_gu)
        pl.when(kind == WRITE_DOWN)(write_down)
        pl.when(kind == OWN)(own_step)
        pl.when(kind == FINISH)(finish)

    for slot in range(2 * CHUNKS):
        partner_send(0, 0, slot).wait_send()
    for t in range(2):
        @pl.loop(0, CHIPS)
        def _(chip, t=t):
            for h in range(CHUNKS):
                pl.when(has_above & (chip <= z))(lambda h=h: send(t, 0, chip, h, partner, False).wait_send())
                pl.when(has_below & (chip >= z))(lambda h=h: send(t, 1, chip, h, partner, False).wait_send())
                send(t, 2, chip, h, partner, False).wait_send()


def put_out(dx, dg, du, dwd, dx_out, dw_gate, dw_up, dw_down, sems):
    depth = dw_gate.shape[0]
    free = pl.ds(free_rows(depth), depth)
    copies = [
        pltpu.make_async_copy(src, dst, sems.at[i])
        for i, (src, dst) in enumerate(((dg.at[free], dw_gate), (du.at[free], dw_up), (dwd, dw_down), (dx, dx_out)))
    ]
    for copy in copies:
        copy.start()
    for copy in copies:
        copy.wait()


def solution(mesh):
    def step(x, dy, gate, up, w_gate, w_up, w_down):
        rows, depth = x.shape
        tokens, width = gate.shape
        bf16 = jnp.bfloat16
        part = rows // CHUNKS
        hbm, vmem = pl.BlockSpec(memory_space=pl.ANY), pl.BlockSpec(memory_space=pltpu.VMEM)
        held = [(rows, depth), (tokens, width), (tokens, width), (width, depth)]
        gathered = [(tokens, depth), (tokens, depth), (CHIPS, rows, depth), (CHIPS, rows, depth), (CHIPS, rows, depth)]
        dma = pltpu.SemaphoreType.DMA
        held_out = pl.pallas_call(
            kernel,
            out_shape=[pltpu.VMEM(s, bf16) for s in held] + [jax.ShapeDtypeStruct(s, bf16) for s in gathered],
            in_specs=[hbm] * 7,
            out_specs=[vmem] * len(held) + [hbm] * len(gathered),
            scratch_shapes=[
                pltpu.VMEM((depth, width), bf16), pltpu.VMEM((depth, width), bf16),
                pltpu.VMEM((depth, width), jnp.float32), pltpu.VMEM((depth, width), jnp.float32),
                pltpu.VMEM((rows, depth), bf16),
                pltpu.VMEM((2, rows, width), bf16), pltpu.VMEM((2, rows, width), bf16), pltpu.VMEM((rows, width), bf16),
                pltpu.VMEM((2 * CHUNKS, part, depth), bf16), pltpu.VMEM((2, part, depth), bf16),
                dma((3,)), dma, dma((2, 2)),
                dma((2, 2 * CHIPS, CHUNKS)), dma((2, 3, CHIPS, CHUNKS)),
                dma((CHIPS, CHUNKS)), dma((CHIPS, CHUNKS * PIECES)), dma((CHIPS, CHUNKS * PIECES)), dma((2 * CHUNKS,)),
            ],
            compiler_params=pltpu.CompilerParams(collective_id=0, has_side_effects=True, vmem_limit_bytes=41 * 2**20),
            cost_estimate=pl.CostEstimate(flops=12 * tokens * depth * width, bytes_accessed=150 * 2**20, transcendentals=0),
        )(x, dy, gate, up, w_gate, w_up, w_down)[: len(held)]
        return pl.pallas_call(
            put_out,
            out_shape=[jax.ShapeDtypeStruct(s, bf16) for s in ((rows, depth), (depth, width), (depth, width), (width, depth))],
            in_specs=[vmem] * len(held),
            out_specs=[hbm] * 4,
            scratch_shapes=[dma((4,))],
            compiler_params=pltpu.CompilerParams(vmem_limit_bytes=2**20),
        )(*held_out)

    whole, rows, cols = P(("dp", "tp"), None), P("tp", None), P(None, "tp")
    return jax.shard_map(
        step,
        mesh=mesh,
        in_specs=(whole, whole, P("dp", "tp"), P("dp", "tp"), cols, cols, rows),
        out_specs=(whole, P("dp", "tp"), P("dp", "tp"), whole),
        check_vma=False,
    )
```

```python
import functools

import jax
import jax.numpy as jnp
from jax import lax
from jax.experimental import pallas as pl
from jax.experimental.pallas import tpu as pltpu
from jax.sharding import PartitionSpec as P

MESH = pl.DeviceIdType.MESH
CHUNKS = 2
PIECES = 2
TILE = 256
CHIPS = 4
NT = (((1,), (1,)), ((), ()))
TN = (((0,), (0,)), ((), ()))
X, FORWARD, REDUCE, WRITE_GU, WRITE_DOWN, OWN, FINISH = range(7)
END_STEPS = (
    (REDUCE, 0), (REDUCE, 1), (WRITE_DOWN, 0), (X, 0), (X, 1), (FORWARD, 1), (X, 2), (X, 3), (REDUCE, 2),
    (FORWARD, 2), (X, 4), (X, 5), (FORWARD, 3), (X, 6), (X, 7), (WRITE_GU, 0), (OWN, 0), (FINISH, 0),
)
MIDDLE_STEPS = (
    (WRITE_DOWN, 0), (X, 0), (X, 1), (FORWARD, 1), (X, 2), (X, 3), (X, 4), (X, 5), (FORWARD, 2),
    (X, 6), (X, 7), (FORWARD, 3), (REDUCE, 0), (REDUCE, 1), (REDUCE, 2), (WRITE_GU, 0), (OWN, 0), (FINISH, 0),
)


def pick(table, i):
    value = jnp.int32(table[0])
    for j in range(1, len(table)):
        value = jnp.where(i == j, jnp.int32(table[j]), value)
    return value


def dot(a, b, dims):
    return lax.dot_general(a, b, dims, preferred_element_type=jnp.float32)


def free_rows(depth):
    z = lax.axis_index("tp") // 2
    return pl.multiple_of(jnp.where(z < CHIPS // 2, depth, 0), depth)


def kernel(
    x, dy, gate, up, w_gate, w_up, w_down,
    dx, dg, du, wd, dy_all, x_all, from_partner, from_below, from_above,
    wg, wu, acc1, acc2, tok, gv, uv, hid, st, terms,
    w_sem, tok_sem, gate_sem, recv_sem, send_sem, partner_sem, below_sem, above_sem, st_sem,
):
    rows, depth = x.shape
    width = gate.shape[1]
    part = rows // CHUNKS
    me = lax.axis_index("tp")
    z, c = me // 2, lax.rem(me, 2)
    other = 1 - c
    last = CHIPS - 1
    is_end = (z == 0) | (z == last)
    low = z < CHIPS // 2
    has_below, has_above = z > 0, z < last
    partner, below, above = {"tp": 2 * z + other}, {"tp": 2 * (z - 1) + c}, {"tp": 2 * (z + 1) + c}

    def mirrored(v):
        return jnp.where(low, v, last - v)

    def arrival(k):
        return mirrored(jnp.where(is_end, k, pick((1, 2, 0, 3), k)))

    def target(r):
        return mirrored(jnp.where(is_end, last - r, pick((3, 0, 2, 1), r)))

    def block_rows(b):
        return pl.ds(pl.multiple_of(b * rows, rows), rows)

    def chunk_rows(b, h):
        return pl.ds(pl.multiple_of(b * rows + h * part, part), part)

    def tile(i, size=TILE):
        return pl.ds(pl.multiple_of(i * size, size), size)

    own = ([st.at[CHUNKS + h] for h in range(CHUNKS)], [x.at[pl.ds(h * part, part)] for h in range(CHUNKS)])
    whole = (dy_all, x_all)

    def send(t, way, chip, h, device, mine):
        b = 2 * chip + c
        src = own[t][h] if mine else whole[t].at[chunk_rows(b, h)]
        return pltpu.make_async_remote_copy(
            src_ref=src,
            dst_ref=whole[t].at[chunk_rows(b, h)],
            send_sem=send_sem.at[t, way, chip, h],
            recv_sem=recv_sem.at[t, b, h],
            device_id=device,
            device_id_type=MESH,
        )

    def await_chunk(t, b, h):
        pltpu.make_async_remote_copy(
            src_ref=whole[t].at[chunk_rows(b, h)],
            dst_ref=whole[t].at[chunk_rows(b, h)],
            send_sem=send_sem.at[t, 0, 0, h],
            recv_sem=recv_sem.at[t, b, h],
            device_id=partner,
            device_id_type=MESH,
        ).wait_recv()

    def send_own(t, ways, before=None):
        for h in range(CHUNKS):
            if before is not None:
                before[h].wait()
            for way, device in enumerate((above, below, partner)):
                if ways[way] is True:
                    send(t, way, z, h, device, True).start()
                elif ways[way] is not False:
                    pl.when(ways[way])(lambda t=t, way=way, h=h, device=device: send(t, way, z, h, device, True).start())

    def forward(t, k, from_below=True, from_above=True):
        for h in range(CHUNKS):
            @pl.when((z - k >= 0) & from_below)
            def _():
                chip = z - k
                await_chunk(t, 2 * chip + c, h)
                pl.when(has_above)(lambda: send(t, 0, chip, h, above, False).start())
                send(t, 2, chip, h, partner, False).start()

            @pl.when((z + k <= last) & from_above)
            def _():
                chip = z + k
                await_chunk(t, 2 * chip + c, h)
                pl.when(has_below)(lambda: send(t, 1, chip, h, below, False).start())
                send(t, 2, chip, h, partner, False).start()

    def sent(t, chip, h):
        pl.when(has_above & (chip <= z))(lambda: send(t, 0, chip, h, partner, False).wait_send())
        pl.when(has_below & (chip >= z))(lambda: send(t, 1, chip, h, partner, False).wait_send())
        send(t, 2, chip, h, partner, False).wait_send()

    def send_x_after(k):
        send_own(1, (has_above & (z == k), has_below & (last - z == k), False))

    mine = [pltpu.make_async_copy(dy.at[pl.ds(h * part, part)], own[0][h], w_sem.at[3 + h]) for h in range(CHUNKS)]
    for copy in mine:
        copy.start()
    barrier = pltpu.get_barrier_semaphore()
    pl.semaphore_signal(barrier, inc=1, device_id=partner, device_id_type=MESH)
    pl.when(has_below)(lambda: pl.semaphore_signal(barrier, inc=1, device_id=below, device_id_type=MESH))
    pl.when(has_above)(lambda: pl.semaphore_signal(barrier, inc=1, device_id=above, device_id_type=MESH))
    pl.semaphore_wait(barrier, jnp.where(is_end, 2, 3))
    send_own(0, (has_above, has_below, True), mine)
    send_x_after(0)
    send_own(1, (False, False, True))

    weights = [pltpu.make_async_copy(a, b, w_sem.at[i]) for i, (a, b) in enumerate(((w_down, wd), (w_gate, wg), (w_up, wu)))]
    for copy in weights:
        copy.start()

    def gate_up(s):
        b = 2 * arrival(s // 2) + jnp.where(lax.rem(s, 2) == 0, c, other)
        slot = lax.rem(s, 2)
        return (
            pltpu.make_async_copy(gate.at[block_rows(b)], gv.at[slot], gate_sem.at[0, slot]),
            pltpu.make_async_copy(up.at[block_rows(b)], uv.at[slot], gate_sem.at[1, slot]),
        )

    for copy in gate_up(jnp.int32(0)):
        copy.start()

    @pl.loop(0, acc1.shape[0] // TILE)
    def _(i):
        acc1[tile(i), :] = jnp.zeros((TILE, width), jnp.float32)

    for copy in weights:
        copy.wait()

    def take_tokens(t, s, b):
        @pl.when(lax.rem(s, 2) == 1)
        def _():
            for h in range(CHUNKS):
                await_chunk(t, b, h)

        @pl.when(s == 0)
        def _():
            pltpu.make_async_copy((dy, x)[t], tok, tok_sem).start()

        @pl.when(s > 0)
        def _():
            pltpu.make_async_copy(whole[t].at[block_rows(b)], tok, tok_sem).start()

        pltpu.make_async_copy((dy, x)[t], tok, tok_sem).wait()

    def partner_send(chip, h, slot):
        return pltpu.make_async_remote_copy(
            src_ref=st.at[slot],
            dst_ref=from_partner.at[chip, pl.ds(h * part, part)],
            send_sem=st_sem.at[slot],
            recv_sem=partner_sem.at[chip, h],
            device_id=partner,
            device_id_type=MESH,
        )

    @pl.loop(0, 2 * CHIPS)
    def _(s):
        k, odd = s // 2, lax.rem(s, 2)
        chip = arrival(k)
        b = 2 * chip + jnp.where(odd == 0, c, other)
        slot = odd

        for j in range(1, CHIPS):
            @pl.when(s == 2 * j)
            def _(j=j):
                forward(0, j)
                send_x_after(j)
                if j == CHIPS - 1:
                    forward(1, 1, z == 1, z == last - 1)

        take_tokens(0, s, b)

        @pl.when(s + 1 < 2 * CHIPS)
        def _():
            for copy in gate_up(s + 1):
                copy.start()

        for copy in gate_up(s):
            copy.wait()

        @pl.loop(0, width // TILE)
        def _(i):
            cols = tile(i)
            d_hidden = dot(tok[...], wd[cols, :], NT)
            g = gv[slot, :, cols].astype(jnp.float32)
            u = uv[slot, :, cols].astype(jnp.float32)
            s_ = jax.nn.sigmoid(g)
            silu = g * s_
            hid[:, cols] = (silu * u).astype(jnp.bfloat16)
            du[block_rows(b), cols] = (d_hidden * silu).astype(jnp.bfloat16)
            dg[block_rows(b), cols] = (d_hidden * u * (s_ * (1.0 + g * (1.0 - s_)))).astype(jnp.bfloat16)

        @pl.loop(0, width // TILE)
        def _(i):
            left = hid[:, tile(i)]
            acc1[tile(i), :] += dot(left, tok[:, :width], TN)
            acc1[pl.ds(pl.multiple_of(width + i * TILE, TILE), TILE), :] += dot(left, tok[:, width:], TN)

        @pl.when(odd == 1)
        def _():
            base = 2 * lax.rem(k, 2)

            @pl.when(k == 1)
            def _():
                for h in range(CHUNKS):
                    sent(0, z, h)

            @pl.when(k >= 2)
            def _():
                for h in range(CHUNKS):
                    partner_send(chip, h, base + h).wait_send()

            @pl.loop(0, depth // TILE)
            def _(i):
                term = dot(dg[block_rows(b), :], wg[tile(i), :], NT) + dot(du[block_rows(b), :], wu[tile(i), :], NT)
                for h in range(CHUNKS):
                    st[base + h, :, tile(i)] = term[h * part:(h + 1) * part].astype(jnp.bfloat16)

            for h in range(CHUNKS):
                partner_send(chip, h, base + h).start()

    def x_step(s):
        chip = arrival(s // 2)
        b = 2 * chip + jnp.where(lax.rem(s, 2) == 0, c, other)
        take_tokens(1, s, b)

        @pl.loop(0, depth // TILE)
        def _(i):
            left = tok[:, tile(i)]
            acc1[tile(i), :] += dot(left, dg[block_rows(b), :], TN)
            acc2[tile(i), :] += dot(left, du[block_rows(b), :], TN)

    fine = part // PIECES

    def arrived(buffer, sem, chip, at, size):
        piece = buffer.at[chip, pl.ds(pl.multiple_of(at * size, size), size)]
        pltpu.make_async_remote_copy(
            src_ref=piece, dst_ref=piece, send_sem=st_sem.at[0], recv_sem=sem.at[chip, at], device_id=partner, device_id_type=MESH
        ).wait_recv()

    def take_term(buffer, chip, at, size, j):
        copy = pltpu.make_async_copy(
            buffer.at[chip, pl.ds(pl.multiple_of(at * size, size), size)], terms.at[j, pl.ds(0, size)], tok_sem
        )
        copy.start()
        copy.wait()

    def own_term(b, h, i):
        here = chunk_rows(b, h)
        return dot(dg[here, :], wg[tile(i), :], NT) + dot(du[here, :], wu[tile(i), :], NT)

    def reduce_step(r):
        chip = target(r)
        b = 2 * chip + c

        @pl.loop(0, CHUNKS)
        def _(h):
            slot = 2 * lax.rem(r, 2) + h
            partner_send(chip, 0, slot).wait_send()
            arrived(from_partner, partner_sem, chip, h, part)
            take_term(from_partner, chip, h, part, 0)
            going_up = chip > z
            for use, buffer, sem in (
                (going_up & has_below, from_below, below_sem),
                (jnp.logical_not(going_up) & has_above, from_above, above_sem),
            ):
                @pl.when(use)
                def _(buffer=buffer, sem=sem):
                    for q in range(PIECES):
                        arrived(buffer, sem, chip, PIECES * h + q, fine)
                    take_term(buffer, chip, h, part, 1)

            @pl.when(is_end)
            def _():
                terms[1] = jnp.zeros((part, depth), jnp.bfloat16)

            @pl.loop(0, depth // TILE)
            def _(i):
                total = own_term(b, h, i)
                for j in range(2):
                    total += terms[j, :, tile(i)].astype(jnp.float32)
                st[slot, :, tile(i)] = total.astype(jnp.bfloat16)

            def pass_on(buffer, sem, device):
                for q in range(PIECES):
                    at = PIECES * h + q
                    pltpu.make_async_remote_copy(
                        src_ref=st.at[slot, pl.ds(q * fine, fine)],
                        dst_ref=buffer.at[chip, pl.ds(pl.multiple_of(at * fine, fine), fine)],
                        send_sem=st_sem.at[slot],
                        recv_sem=sem.at[chip, at],
                        device_id=device,
                        device_id_type=MESH,
                    ).start()

            pl.when(going_up)(lambda: pass_on(from_below, below_sem, above))
            pl.when(jnp.logical_not(going_up))(lambda: pass_on(from_above, above_sem, below))

    def halves(i):
        return lax.rem(i, width // TILE), (i // (width // TILE)) * rows

    def own_step():
        @pl.loop(0, CHUNKS)
        def _(h):
            arrived(from_partner, partner_sem, z, h, part)
            take_term(from_partner, z, h, part, 0)

            @pl.loop(0, depth // TILE)
            def _(i):
                column, down = halves(i)
                total = own_term(me, h, i) + terms[0, :, tile(i)].astype(jnp.float32)
                acc1[pl.ds(pl.multiple_of(down + h * part, part), part), tile(column)] = total

        @pl.loop(0, CHIPS)
        def _(chip):
            for h in range(CHUNKS):
                pl.when(chip != z)(lambda h=h: sent(0, chip, h))
                sent(1, chip, h)

    def finish():
        for at in range(CHUNKS * PIECES):
            for j, (use, buffer, sem) in enumerate(((has_below, from_below, below_sem), (has_above, from_above, above_sem))):
                @pl.when(use)
                def _(j=j, buffer=buffer, sem=sem):
                    arrived(buffer, sem, z, at, fine)
                    take_term(buffer, z, at, fine, j)
                    for side in range(2):
                        here = pl.ds(side * rows + at * fine, fine)
                        acc1[here, :] += terms[j, :fine, side * width:(side + 1) * width].astype(jnp.float32)
            for side in range(2):
                here = pl.ds(side * rows + at * fine, fine)
                dx[at * fine:(at + 1) * fine, side * width:(side + 1) * width] = acc1[here, :].astype(jnp.bfloat16)

    def write_down():
        for side in range(2):
            wd[:, side * width:(side + 1) * width] = acc1[side * width:(side + 1) * width, :].astype(jnp.bfloat16)

        @pl.loop(0, depth // TILE)
        def _(i):
            acc1[tile(i), :] = jnp.zeros((TILE, width), jnp.float32)
            acc2[tile(i), :] = jnp.zeros((TILE, width), jnp.float32)

    def write_gu():
        free = free_rows(depth)

        @pl.loop(0, depth // TILE)
        def _(i):
            there = pl.ds(pl.multiple_of(free + i * TILE, TILE), TILE)
            dg[there, :] = acc1[tile(i), :].astype(jnp.bfloat16)
            du[there, :] = acc2[tile(i), :].astype(jnp.bfloat16)

    @pl.loop(0, len(END_STEPS))
    def _(t):
        kind = jnp.where(is_end, pick([s[0] for s in END_STEPS], t), pick([s[0] for s in MIDDLE_STEPS], t))
        arg = jnp.where(is_end, pick([s[1] for s in END_STEPS], t), pick([s[1] for s in MIDDLE_STEPS], t))
        pl.when(kind == X)(lambda: x_step(arg))
        pl.when((kind == FORWARD) & (arg == 1))(lambda: forward(1, 1, z != 1, z != last - 1))
        for k in range(2, CHIPS):
            pl.when((kind == FORWARD) & (arg == k))(lambda k=k: forward(1, k))
        pl.when(kind == REDUCE)(lambda: reduce_step(arg))
        pl.when(kind == WRITE_GU)(write_gu)
        pl.when(kind == WRITE_DOWN)(write_down)
        pl.when(kind == OWN)(own_step)
        pl.when(kind == FINISH)(finish)

    for slot in range(2 * CHUNKS):
        partner_send(0, 0, slot).wait_send()


def put_out(dx, dg, du, dwd, dx_out, dw_gate, dw_up, dw_down, sems):
    depth = dw_gate.shape[0]
    free = pl.ds(free_rows(depth), depth)
    copies = [
        pltpu.make_async_copy(src, dst, sems.at[i])
        for i, (src, dst) in enumerate(((dg.at[free], dw_gate), (du.at[free], dw_up), (dwd, dw_down), (dx, dx_out)))
    ]
    for copy in copies:
        copy.start()
    for copy in copies:
        copy.wait()


def solution(mesh):
    def step(x, dy, gate, up, w_gate, w_up, w_down):
        rows, depth = x.shape
        tokens, width = gate.shape
        bf16 = jnp.bfloat16
        part = rows // CHUNKS
        hbm, vmem = pl.BlockSpec(memory_space=pl.ANY), pl.BlockSpec(memory_space=pltpu.VMEM)
        held = [(rows, depth), (tokens, width), (tokens, width), (width, depth)]
        gathered = [(tokens, depth), (tokens, depth), (CHIPS, rows, depth), (CHIPS, rows, depth), (CHIPS, rows, depth)]
        dma = pltpu.SemaphoreType.DMA
        held_out = pl.pallas_call(
            kernel,
            out_shape=[pltpu.VMEM(s, bf16) for s in held] + [jax.ShapeDtypeStruct(s, bf16) for s in gathered],
            in_specs=[hbm] * 7,
            out_specs=[vmem] * len(held) + [hbm] * len(gathered),
            scratch_shapes=[
                pltpu.VMEM((depth, width), bf16), pltpu.VMEM((depth, width), bf16),
                pltpu.VMEM((depth, width), jnp.float32), pltpu.VMEM((depth, width), jnp.float32),
                pltpu.VMEM((rows, depth), bf16),
                pltpu.VMEM((2, rows, width), bf16), pltpu.VMEM((2, rows, width), bf16), pltpu.VMEM((rows, width), bf16),
                pltpu.VMEM((2 * CHUNKS, part, depth), bf16), pltpu.VMEM((2, part, depth), bf16),
                dma((3 + CHUNKS,)), dma, dma((2, 2)),
                dma((2, 2 * CHIPS, CHUNKS)), dma((2, 3, CHIPS, CHUNKS)),
                dma((CHIPS, CHUNKS)), dma((CHIPS, CHUNKS * PIECES)), dma((CHIPS, CHUNKS * PIECES)), dma((2 * CHUNKS,)),
            ],
            compiler_params=pltpu.CompilerParams(collective_id=0, has_side_effects=True, vmem_limit_bytes=41 * 2**20),
            cost_estimate=pl.CostEstimate(flops=12 * tokens * depth * width, bytes_accessed=150 * 2**20, transcendentals=0),
        )(x, dy, gate, up, w_gate, w_up, w_down)[: len(held)]
        return pl.pallas_call(
            put_out,
            out_shape=[jax.ShapeDtypeStruct(s, bf16) for s in ((rows, depth), (depth, width), (depth, width), (width, depth))],
            in_specs=[vmem] * len(held),
            out_specs=[hbm] * 4,
            scratch_shapes=[dma((4,))],
            compiler_params=pltpu.CompilerParams(vmem_limit_bytes=2**20),
        )(*held_out)

    whole, rows, cols = P(("dp", "tp"), None), P("tp", None), P(None, "tp")
    return jax.shard_map(
        step,
        mesh=mesh,
        in_specs=(whole, whole, P("dp", "tp"), P("dp", "tp"), cols, cols, rows),
        out_specs=(whole, P("dp", "tp"), P("dp", "tp"), whole),
        check_vma=False,
    )
```

```python
import functools

import jax
import jax.numpy as jnp
from jax import lax
from jax.experimental import pallas as pl
from jax.experimental.pallas import tpu as pltpu
from jax.sharding import PartitionSpec as P

MESH = pl.DeviceIdType.MESH
CHUNKS = 2
PIECES = 2
TILE = 256
CHIPS = 4
NT = (((1,), (1,)), ((), ()))
TN = (((0,), (0,)), ((), ()))
X, FORWARD, REDUCE, WRITE_GU, WRITE_DOWN, OWN, FINISH = range(7)
END_STEPS = (
    (REDUCE, 0), (REDUCE, 1), (WRITE_DOWN, 0), (X, 0), (X, 1), (FORWARD, 1), (X, 2), (X, 3), (REDUCE, 2),
    (FORWARD, 2), (X, 4), (X, 5), (FORWARD, 3), (X, 6), (X, 7), (WRITE_GU, 0), (OWN, 0), (FINISH, 0),
)
MIDDLE_STEPS = (
    (WRITE_DOWN, 0), (X, 0), (X, 1), (FORWARD, 1), (X, 2), (X, 3), (X, 4), (X, 5), (FORWARD, 2),
    (X, 6), (X, 7), (FORWARD, 3), (REDUCE, 0), (REDUCE, 1), (REDUCE, 2), (WRITE_GU, 0), (OWN, 0), (FINISH, 0),
)


def pick(table, i):
    value = jnp.int32(table[0])
    for j in range(1, len(table)):
        value = jnp.where(i == j, jnp.int32(table[j]), value)
    return value


def dot(a, b, dims):
    return lax.dot_general(a, b, dims, preferred_element_type=jnp.float32)


def free_rows(depth):
    z = lax.axis_index("tp") // 2
    return pl.multiple_of(jnp.where(z < CHIPS // 2, depth, 0), depth)


def kernel(
    x, dy, gate, up, w_gate, w_up, w_down,
    dx, dg, du, wd, last_own, last_below, last_above, dy_all, x_all, from_partner, from_below, from_above,
    wg, wu, acc1, acc2, tok, gv, uv, hid, st, terms,
    w_sem, tok_sem, gate_sem, recv_sem, send_sem, partner_sem, below_sem, above_sem, st_sem,
):
    rows, depth = x.shape
    width = gate.shape[1]
    part = rows // CHUNKS
    me = lax.axis_index("tp")
    z, c = me // 2, lax.rem(me, 2)
    other = 1 - c
    last = CHIPS - 1
    is_end = (z == 0) | (z == last)
    low = z < CHIPS // 2
    has_below, has_above = z > 0, z < last
    partner, below, above = {"tp": 2 * z + other}, {"tp": 2 * (z - 1) + c}, {"tp": 2 * (z + 1) + c}

    def mirrored(v):
        return jnp.where(low, v, last - v)

    def arrival(k):
        return mirrored(jnp.where(is_end, k, pick((1, 2, 0, 3), k)))

    def target(r):
        return mirrored(jnp.where(is_end, last - r, pick((3, 0, 2, 1), r)))

    def block_rows(b):
        return pl.ds(pl.multiple_of(b * rows, rows), rows)

    def chunk_rows(b, h):
        return pl.ds(pl.multiple_of(b * rows + h * part, part), part)

    def tile(i, size=TILE):
        return pl.ds(pl.multiple_of(i * size, size), size)

    own = ([st.at[CHUNKS + h] for h in range(CHUNKS)], [x.at[pl.ds(h * part, part)] for h in range(CHUNKS)])
    whole = (dy_all, x_all)

    def send(t, way, chip, h, device, mine):
        b = 2 * chip + c
        src = own[t][h] if mine else whole[t].at[chunk_rows(b, h)]
        return pltpu.make_async_remote_copy(
            src_ref=src,
            dst_ref=whole[t].at[chunk_rows(b, h)],
            send_sem=send_sem.at[t, way, chip, h],
            recv_sem=recv_sem.at[t, b, h],
            device_id=device,
            device_id_type=MESH,
        )

    def await_chunk(t, b, h):
        pltpu.make_async_remote_copy(
            src_ref=whole[t].at[chunk_rows(b, h)],
            dst_ref=whole[t].at[chunk_rows(b, h)],
            send_sem=send_sem.at[t, 0, 0, h],
            recv_sem=recv_sem.at[t, b, h],
            device_id=partner,
            device_id_type=MESH,
        ).wait_recv()

    def send_own(t, ways, before=None):
        for h in range(CHUNKS):
            if before is not None:
                before[h].wait()
            for way, device in enumerate((above, below, partner)):
                if ways[way] is True:
                    send(t, way, z, h, device, True).start()
                elif ways[way] is not False:
                    pl.when(ways[way])(lambda t=t, way=way, h=h, device=device: send(t, way, z, h, device, True).start())

    def forward(t, k, from_below=True, from_above=True):
        for h in range(CHUNKS):
            @pl.when((z - k >= 0) & from_below)
            def _():
                chip = z - k
                await_chunk(t, 2 * chip + c, h)
                pl.when(has_above)(lambda: send(t, 0, chip, h, above, False).start())
                send(t, 2, chip, h, partner, False).start()

            @pl.when((z + k <= last) & from_above)
            def _():
                chip = z + k
                await_chunk(t, 2 * chip + c, h)
                pl.when(has_below)(lambda: send(t, 1, chip, h, below, False).start())
                send(t, 2, chip, h, partner, False).start()

    def sent(t, chip, h):
        pl.when(has_above & (chip <= z))(lambda: send(t, 0, chip, h, partner, False).wait_send())
        pl.when(has_below & (chip >= z))(lambda: send(t, 1, chip, h, partner, False).wait_send())
        send(t, 2, chip, h, partner, False).wait_send()

    def send_x_after(k):
        send_own(1, (has_above & (z == k), has_below & (last - z == k), False))

    mine = [pltpu.make_async_copy(dy.at[pl.ds(h * part, part)], own[0][h], w_sem.at[3 + h]) for h in range(CHUNKS)]
    for copy in mine:
        copy.start()
    barrier = pltpu.get_barrier_semaphore()
    pl.semaphore_signal(barrier, inc=1, device_id=partner, device_id_type=MESH)
    pl.when(has_below)(lambda: pl.semaphore_signal(barrier, inc=1, device_id=below, device_id_type=MESH))
    pl.when(has_above)(lambda: pl.semaphore_signal(barrier, inc=1, device_id=above, device_id_type=MESH))
    pl.semaphore_wait(barrier, jnp.where(is_end, 2, 3))
    send_own(0, (has_above, has_below, True), mine)
    send_x_after(0)
    send_own(1, (False, False, True))

    weights = [pltpu.make_async_copy(a, b, w_sem.at[i]) for i, (a, b) in enumerate(((w_down, wd), (w_gate, wg), (w_up, wu)))]
    for copy in weights:
        copy.start()

    def gate_up(s):
        b = 2 * arrival(s // 2) + jnp.where(lax.rem(s, 2) == 0, c, other)
        slot = lax.rem(s, 2)
        return (
            pltpu.make_async_copy(gate.at[block_rows(b)], gv.at[slot], gate_sem.at[0, slot]),
            pltpu.make_async_copy(up.at[block_rows(b)], uv.at[slot], gate_sem.at[1, slot]),
        )

    for copy in gate_up(jnp.int32(0)):
        copy.start()

    @pl.loop(0, acc1.shape[0] // TILE)
    def _(i):
        acc1[tile(i), :] = jnp.zeros((TILE, width), jnp.float32)

    for copy in weights:
        copy.wait()

    def take_tokens(t, s, b):
        @pl.when(lax.rem(s, 2) == 1)
        def _():
            for h in range(CHUNKS):
                await_chunk(t, b, h)

        @pl.when(s == 0)
        def _():
            pltpu.make_async_copy((dy, x)[t], tok, tok_sem).start()

        @pl.when(s > 0)
        def _():
            pltpu.make_async_copy(whole[t].at[block_rows(b)], tok, tok_sem).start()

        pltpu.make_async_copy((dy, x)[t], tok, tok_sem).wait()

    def partner_send(chip, h, slot):
        return pltpu.make_async_remote_copy(
            src_ref=st.at[slot],
            dst_ref=from_partner.at[chip, pl.ds(h * part, part)],
            send_sem=st_sem.at[slot],
            recv_sem=partner_sem.at[chip, h],
            device_id=partner,
            device_id_type=MESH,
        )

    @pl.loop(0, 2 * CHIPS)
    def _(s):
        k, odd = s // 2, lax.rem(s, 2)
        chip = arrival(k)
        b = 2 * chip + jnp.where(odd == 0, c, other)
        slot = odd

        for j in range(1, CHIPS):
            @pl.when(s == 2 * j)
            def _(j=j):
                forward(0, j)
                send_x_after(j)
                if j == CHIPS - 1:
                    forward(1, 1, z == 1, z == last - 1)

        take_tokens(0, s, b)

        @pl.when(s + 1 < 2 * CHIPS)
        def _():
            for copy in gate_up(s + 1):
                copy.start()

        for copy in gate_up(s):
            copy.wait()

        @pl.loop(0, width // TILE)
        def _(i):
            cols = tile(i)
            d_hidden = dot(tok[...], wd[cols, :], NT)
            g = gv[slot, :, cols].astype(jnp.float32)
            u = uv[slot, :, cols].astype(jnp.float32)
            s_ = jax.nn.sigmoid(g)
            silu = g * s_
            hid[:, cols] = (silu * u).astype(jnp.bfloat16)
            du[block_rows(b), cols] = (d_hidden * silu).astype(jnp.bfloat16)
            dg[block_rows(b), cols] = (d_hidden * u * (s_ * (1.0 + g * (1.0 - s_)))).astype(jnp.bfloat16)

        @pl.loop(0, width // TILE)
        def _(i):
            left = hid[:, tile(i)]
            acc1[tile(i), :] += dot(left, tok[:, :width], TN)
            acc1[pl.ds(pl.multiple_of(width + i * TILE, TILE), TILE), :] += dot(left, tok[:, width:], TN)

        @pl.when(odd == 1)
        def _():
            base = 2 * lax.rem(k, 2)

            @pl.when(k == 1)
            def _():
                for h in range(CHUNKS):
                    sent(0, z, h)

            @pl.when(k >= 2)
            def _():
                for h in range(CHUNKS):
                    partner_send(chip, h, base + h).wait_send()

            @pl.loop(0, depth // TILE)
            def _(i):
                term = dot(dg[block_rows(b), :], wg[tile(i), :], NT) + dot(du[block_rows(b), :], wu[tile(i), :], NT)
                for h in range(CHUNKS):
                    st[base + h, :, tile(i)] = term[h * part:(h + 1) * part].astype(jnp.bfloat16)

            for h in range(CHUNKS):
                partner_send(chip, h, base + h).start()

    def x_step(s):
        chip = arrival(s // 2)
        b = 2 * chip + jnp.where(lax.rem(s, 2) == 0, c, other)
        take_tokens(1, s, b)

        @pl.loop(0, depth // TILE)
        def _(i):
            left = tok[:, tile(i)]
            acc1[tile(i), :] += dot(left, dg[block_rows(b), :], TN)
            acc2[tile(i), :] += dot(left, du[block_rows(b), :], TN)

    fine = part // PIECES

    def arrived(buffer, sem, chip, at, size):
        piece = buffer.at[chip, pl.ds(pl.multiple_of(at * size, size), size)]
        pltpu.make_async_remote_copy(
            src_ref=piece, dst_ref=piece, send_sem=st_sem.at[0], recv_sem=sem.at[chip, at], device_id=partner, device_id_type=MESH
        ).wait_recv()

    def take_term(buffer, chip, at, size, j):
        copy = pltpu.make_async_copy(
            buffer.at[chip, pl.ds(pl.multiple_of(at * size, size), size)], terms.at[j, pl.ds(0, size)], tok_sem
        )
        copy.start()
        copy.wait()

    def own_term(b, h, i):
        here = chunk_rows(b, h)
        return dot(dg[here, :], wg[tile(i), :], NT) + dot(du[here, :], wu[tile(i), :], NT)

    def reduce_step(r):
        chip = target(r)
        b = 2 * chip + c

        @pl.loop(0, CHUNKS)
        def _(h):
            slot = 2 * lax.rem(r, 2) + h
            partner_send(chip, 0, slot).wait_send()
            arrived(from_partner, partner_sem, chip, h, part)
            take_term(from_partner, chip, h, part, 0)
            going_up = chip > z
            for use, buffer, sem in (
                (going_up & has_below, from_below, below_sem),
                (jnp.logical_not(going_up) & has_above, from_above, above_sem),
            ):
                @pl.when(use)
                def _(buffer=buffer, sem=sem):
                    for q in range(PIECES):
                        arrived(buffer, sem, chip, PIECES * h + q, fine)
                    take_term(buffer, chip, h, part, 1)

            @pl.when(is_end)
            def _():
                terms[1] = jnp.zeros((part, depth), jnp.bfloat16)

            @pl.loop(0, depth // TILE)
            def _(i):
                total = own_term(b, h, i)
                for j in range(2):
                    total += terms[j, :, tile(i)].astype(jnp.float32)
                st[slot, :, tile(i)] = total.astype(jnp.bfloat16)

            def pass_on(buffer, sem, device, landing, is_final):
                for q in range(PIECES):
                    at = PIECES * h + q

                    def start(dst, q=q, at=at):
                        pltpu.make_async_remote_copy(
                            src_ref=st.at[slot, pl.ds(q * fine, fine)],
                            dst_ref=dst,
                            send_sem=st_sem.at[slot],
                            recv_sem=sem.at[chip, at],
                            device_id=device,
                            device_id_type=MESH,
                        ).start()

                    piece = buffer.at[chip, pl.ds(pl.multiple_of(at * fine, fine), fine)]
                    if q < PIECES - 1:
                        start(piece)
                    else:
                        to_vmem = is_final & (h == CHUNKS - 1)
                        pl.when(to_vmem)(lambda start=start: start(landing))
                        pl.when(jnp.logical_not(to_vmem))(lambda start=start, piece=piece: start(piece))

            pl.when(going_up)(lambda: pass_on(from_below, below_sem, above, last_below, chip == z + 1))
            pl.when(jnp.logical_not(going_up))(lambda: pass_on(from_above, above_sem, below, last_above, chip == z - 1))

    def halves(i):
        return lax.rem(i, width // TILE), (i // (width // TILE)) * rows

    def own_step():
        @pl.loop(0, CHUNKS)
        def _(h):
            arrived(from_partner, partner_sem, z, h, part)
            take_term(from_partner, z, h, part, 0)

            @pl.loop(0, depth // TILE)
            def _(i):
                column, down = halves(i)
                total = own_term(me, h, i) + terms[0, :, tile(i)].astype(jnp.float32)
                acc1[pl.ds(pl.multiple_of(down + h * part, part), part), tile(column)] = total

        @pl.loop(0, CHIPS)
        def _(chip):
            for h in range(CHUNKS):
                pl.when(chip != z)(lambda h=h: sent(0, chip, h))
                sent(1, chip, h)

    def finish():
        pieces = CHUNKS * PIECES
        sides = ((has_below, from_below, below_sem, last_below), (has_above, from_above, above_sem, last_above))
        for side in range(2):
            last_own[:, side * width:(side + 1) * width] = acc1[pl.ds(side * rows + (pieces - 1) * fine, fine), :]
        for at in range(pieces - 1):
            for j, (use, buffer, sem, _) in enumerate(sides):
                @pl.when(use)
                def _(j=j, buffer=buffer, sem=sem):
                    arrived(buffer, sem, z, at, fine)
                    take_term(buffer, z, at, fine, j)
                    for side in range(2):
                        here = pl.ds(side * rows + at * fine, fine)
                        acc1[here, :] += terms[j, :fine, side * width:(side + 1) * width].astype(jnp.float32)
            for side in range(2):
                here = pl.ds(side * rows + at * fine, fine)
                dx[at * fine:(at + 1) * fine, side * width:(side + 1) * width] = acc1[here, :].astype(jnp.bfloat16)
        for use, _, sem, landing in sides:
            pl.when(use)(
                lambda sem=sem, landing=landing: pltpu.make_async_remote_copy(
                    src_ref=landing, dst_ref=landing, send_sem=st_sem.at[0], recv_sem=sem.at[z, pieces - 1],
                    device_id=partner, device_id_type=MESH,
                ).wait_recv()
            )

    def write_down():
        for side in range(2):
            wd[:, side * width:(side + 1) * width] = acc1[side * width:(side + 1) * width, :].astype(jnp.bfloat16)

        @pl.loop(0, depth // TILE)
        def _(i):
            acc1[tile(i), :] = jnp.zeros((TILE, width), jnp.float32)
            acc2[tile(i), :] = jnp.zeros((TILE, width), jnp.float32)

    def write_gu():
        free = free_rows(depth)

        @pl.loop(0, depth // TILE)
        def _(i):
            there = pl.ds(pl.multiple_of(free + i * TILE, TILE), TILE)
            dg[there, :] = acc1[tile(i), :].astype(jnp.bfloat16)
            du[there, :] = acc2[tile(i), :].astype(jnp.bfloat16)

    @pl.loop(0, len(END_STEPS))
    def _(t):
        kind = jnp.where(is_end, pick([s[0] for s in END_STEPS], t), pick([s[0] for s in MIDDLE_STEPS], t))
        arg = jnp.where(is_end, pick([s[1] for s in END_STEPS], t), pick([s[1] for s in MIDDLE_STEPS], t))
        pl.when(kind == X)(lambda: x_step(arg))
        pl.when((kind == FORWARD) & (arg == 1))(lambda: forward(1, 1, z != 1, z != last - 1))
        for k in range(2, CHIPS):
            pl.when((kind == FORWARD) & (arg == k))(lambda k=k: forward(1, k))
        pl.when(kind == REDUCE)(lambda: reduce_step(arg))
        pl.when(kind == WRITE_GU)(write_gu)
        pl.when(kind == WRITE_DOWN)(write_down)
        pl.when(kind == OWN)(own_step)
        pl.when(kind == FINISH)(finish)

    for slot in range(2 * CHUNKS):
        partner_send(0, 0, slot).wait_send()


def put_out(dx, dg, du, dwd, last_own, last_below, last_above, dx_out, dw_gate, dw_up, dw_down, last, sems):
    depth = dw_gate.shape[0]
    head = dx.shape[0] - last.shape[0]
    z = lax.axis_index("tp") // 2
    free = pl.ds(free_rows(depth), depth)
    pairs = (
        (dg.at[free], dw_gate), (du.at[free], dw_up), (dwd, dw_down),
        (dx.at[:head], dx_out.at[:head]), (last, dx_out.at[head:]),
    )
    copies = [pltpu.make_async_copy(src, dst, sems.at[i]) for i, (src, dst) in enumerate(pairs)]
    for copy in copies[:-1]:
        copy.start()
    for case, terms in (
        (z == 0, (last_above,)),
        (z == CHIPS - 1, (last_below,)),
        ((z > 0) & (z < CHIPS - 1), (last_below, last_above)),
    ):
        @pl.when(case)
        def _(terms=terms):
            total = last_own[...]
            for term in terms:
                total += term[...].astype(jnp.float32)
            last[...] = total.astype(jnp.bfloat16)

    copies[-1].start()
    for copy in copies:
        copy.wait()


def solution(mesh):
    def step(x, dy, gate, up, w_gate, w_up, w_down):
        rows, depth = x.shape
        tokens, width = gate.shape
        bf16 = jnp.bfloat16
        part = rows // CHUNKS
        hbm, vmem = pl.BlockSpec(memory_space=pl.ANY), pl.BlockSpec(memory_space=pltpu.VMEM)
        fine = part // PIECES
        held = [pltpu.VMEM(s, bf16) for s in ((rows, depth), (tokens, width), (tokens, width), (width, depth))]
        held += [pltpu.VMEM((fine, depth), t) for t in (jnp.float32, bf16, bf16)]
        gathered = [(tokens, depth), (tokens, depth), (CHIPS, rows, depth), (CHIPS, rows, depth), (CHIPS, rows, depth)]
        dma = pltpu.SemaphoreType.DMA
        held_out = pl.pallas_call(
            kernel,
            out_shape=held + [jax.ShapeDtypeStruct(s, bf16) for s in gathered],
            in_specs=[hbm] * 7,
            out_specs=[vmem] * len(held) + [hbm] * len(gathered),
            scratch_shapes=[
                pltpu.VMEM((depth, width), bf16), pltpu.VMEM((depth, width), bf16),
                pltpu.VMEM((depth, width), jnp.float32), pltpu.VMEM((depth, width), jnp.float32),
                pltpu.VMEM((rows, depth), bf16),
                pltpu.VMEM((2, rows, width), bf16), pltpu.VMEM((2, rows, width), bf16), pltpu.VMEM((rows, width), bf16),
                pltpu.VMEM((2 * CHUNKS, part, depth), bf16), pltpu.VMEM((2, part, depth), bf16),
                dma((3 + CHUNKS,)), dma, dma((2, 2)),
                dma((2, 2 * CHIPS, CHUNKS)), dma((2, 3, CHIPS, CHUNKS)),
                dma((CHIPS, CHUNKS)), dma((CHIPS, CHUNKS * PIECES)), dma((CHIPS, CHUNKS * PIECES)), dma((2 * CHUNKS,)),
            ],
            compiler_params=pltpu.CompilerParams(collective_id=0, has_side_effects=True, vmem_limit_bytes=79 * 2**19),
            cost_estimate=pl.CostEstimate(flops=12 * tokens * depth * width, bytes_accessed=150 * 2**20, transcendentals=0),
        )(x, dy, gate, up, w_gate, w_up, w_down)[: len(held)]
        return pl.pallas_call(
            put_out,
            out_shape=[jax.ShapeDtypeStruct(s, bf16) for s in ((rows, depth), (depth, width), (depth, width), (width, depth))],
            in_specs=[vmem] * len(held),
            out_specs=[hbm] * 4,
            scratch_shapes=[pltpu.VMEM((fine, depth), bf16), dma((5,))],
            compiler_params=pltpu.CompilerParams(vmem_limit_bytes=2 * 2**20),
        )(*held_out)

    whole, rows, cols = P(("dp", "tp"), None), P("tp", None), P(None, "tp")
    return jax.shard_map(
        step,
        mesh=mesh,
        in_specs=(whole, whole, P("dp", "tp"), P("dp", "tp"), cols, cols, rows),
        out_specs=(whole, P("dp", "tp"), P("dp", "tp"), whole),
        check_vma=False,
    )
```
